128 devices in a mesh: row: 8 (over z, y_hi), col: 16 (over y_lo, x, core).
Axes of the slice: x: 4, y: 4 (y_hi: 2, y_lo: 2; y = y_hi * 2 + y_lo), z: 4, core: 2. Of those that a mesh axis runs over, the one named last changes fastest.
Arguments:
- green: float32 [2048, 16384], P(('row', 'col')), may hold values from -0.1875 to 0.1875
- noise_precision: float32 [2048], P(('row', 'col')), may hold values from 0.5 to 4
- data_set: int32 [2048], P(('row', 'col')), may hold values from 0 to 3
- set_scale: float32 [4], replicated, may hold values from 0.5 to 2
- stiffness: float32 [8192], replicated, may hold values from 0.25 to 2
- patch_cell: int32 [8192], replicated, may hold values from 0 to 8191, each once
Outputs:
- precision_matrix: float32 [16384, 16384], P('row', 'col')
The draws below stay inside these ranges and needn't reach their ends.
Inputs may be any that keep to these rules, and one draw needn't show every extreme that they name: `patch_cell`: every cell 0 to 8191 holds exactly one patch.
All inputs are finite; a program needn't handle non-finite values.
Results may differ from the reference program's by a relative error of at most 0.00005.
Values sent between devices are 32-bit elements; how exact they have to be, the bound alone decides.
No kernel may reach another device: no remote copies, remote signals or barrier semaphores. Data moves between devices by JAX's collectives and lax.ppermute only.
A program may use at most 256 MiB of HBM per device.

```python
import math
import jax
import jax.numpy as jnp
from jax import lax

NSTRIKE = 128
NDIP = 64
NSETS = 4
O = 2048
P_SIZE = 8192
M = 16384


def place_ends(entries, stream_key, least, high):
    shape = entries.shape
    place = [jax.random.randint(jax.random.fold_in(stream_key, axis), (), 0, shape[axis]) for axis in range(len(shape))]
    entries = entries.at[tuple(place)].set(least)
    longest = shape.index(max(shape))
    place[longest] = (place[longest] + 1) % shape[longest]
    return entries.at[tuple(place)].set(high)


def levels(rng, shape, cuts, low, largest):
    def one(position, blocks):
        draws = jax.random.uniform(jax.random.fold_in(jax.random.fold_in(rng, 6), position), (blocks,), jnp.float32, low / len(cuts), largest / len(cuts))
        return jnp.repeat(jnp.exp(draws), shape[position] // blocks).reshape((-1,) + (1,) * (len(shape) - position - 1))

    level = one(*cuts[0])
    for cut in cuts[1:]:
        level = level * one(*cut)
    return level


def gaussian(key, extent, scale, bound, cuts=(), kind=jnp.bfloat16):
    result = scale * jax.random.normal(key, extent, jnp.float32)
    if cuts:
        result = result * levels(key, extent, cuts, -0.22, 0.18)
    return jnp.clip(result, -bound, bound).astype(kind)


def setup_inputs(seed: int = 0) -> dict:
    splits = jax.random.split(jax.random.key(seed), 7)
    return {
        "green": gaussian(splits[0], (O, M), (O // 2) ** -0.5, 0.1875, ((0, 128),), jnp.float32),
        "noise_precision": jnp.clip(jnp.exp(math.log(4.0) - 2.0794415 * jax.random.uniform(splits[1], (O,), jnp.float32) ** levels(splits[1], (O,), ((0, 128),), -0.2, 0.2)), 0.5, 4.0),
        "data_set": place_ends(jax.random.randint(splits[2], (O,), 0, NSETS), jax.random.fold_in(splits[2], 1), 0, NSETS - 1).astype(jnp.int32),
        "set_scale": jnp.clip(jnp.exp(jax.random.uniform(splits[3], (NSETS,), jnp.float32, math.log(0.5), math.log(2.0))), 0.5, 2.0),
        "stiffness": jnp.clip(jnp.exp(jax.random.uniform(splits[4], (P_SIZE,), jnp.float32, math.log(0.25), math.log(2.0))), 0.25, 2.0),
        "patch_cell": jax.random.permutation(splits[5], P_SIZE).astype(jnp.int32),
    }


def reference(green, noise_precision, data_set, set_scale, stiffness, patch_cell):
    weight = noise_precision * set_scale[data_set]
    scaled = green * jnp.sqrt(weight)[:, None]
    precision_matrix = lax.dot_general(scaled, scaled, (((0,), (0,)), ((), ())), precision=lax.Precision.HIGHEST, preferred_element_type=jnp.float32)
    patch_count = NSTRIKE * NDIP
    cell_ids = jnp.arange(patch_count, dtype=jnp.int32)
    owner = jnp.zeros((patch_count,), jnp.int32).at[patch_cell].set(cell_ids)
    strike_pos = cell_ids // NDIP
    dip_pos = cell_ids % NDIP
    along = owner[jnp.minimum(cell_ids + NDIP, patch_count - 1)]
    below = owner[jnp.minimum(cell_ids + 1, patch_count - 1)]
    heads = jnp.concatenate([owner, owner])
    tails = jnp.concatenate([along, below])
    valid = jnp.concatenate([strike_pos < NSTRIKE - 1, dip_pos < NDIP - 1])
    edges = jnp.where(valid, 0.5 * (stiffness[heads] + stiffness[tails]), 0.0)
    row_list = []
    col_list = []
    values = []
    for component in range(2):
        first_ids = (component * patch_count + heads).astype(jnp.int32)
        second_ids = (component * patch_count + tails).astype(jnp.int32)
        row_list += [first_ids, second_ids, first_ids, second_ids]
        col_list += [second_ids, first_ids, first_ids, second_ids]
        values += [-edges, -edges, edges, edges]
    return precision_matrix.at[jnp.concatenate(row_list), jnp.concatenate(col_list)].add(jnp.concatenate(values))
```

```python
import functools

import jax
import jax.numpy as jnp
from jax import lax
from jax.experimental import pallas as pl
from jax.experimental.pallas import tpu as pltpu
from jax.sharding import PartitionSpec as P


NSTRIKE = 128
NDIP = 64
AXES = ("row", "col")
CROSS = (3, 2, 1, 0)
PAIR = (1, 0, 3, 2)
DIAGONAL = (2, 3, 0, 1)
ROWS = 2048
COLS = 1024
PATCHES = 8192


def place(index):
    row, col = divmod(index, 16)
    z, y_hi = divmod(row, 2)
    y_lo, rest = divmod(col, 8)
    x, core = divmod(rest, 2)
    return z, 2 * y_hi + y_lo, x, core


def device(z, y, x, core):
    return (z % 4 * 2 + y // 2) * 16 + (y % 2) * 8 + x % 4 * 2 + core


def send(block, target):
    pairs = [(index, device(*target(*place(index)))) for index in range(128)]
    return lax.ppermute(block, AXES, pairs)


def kernel_call(body, outs, args, in_specs=None, flops=0, nbytes=0, scratch=(), limit=6, **extra):
    return pl.pallas_call(
        body,
        out_shape=outs,
        in_specs=in_specs or [VMEM] * len(args),
        scratch_shapes=scratch,
        cost_estimate=pl.CostEstimate(flops=flops, bytes_accessed=nbytes, transcendentals=0),
        compiler_params=pltpu.CompilerParams(vmem_limit_bytes=limit << 20),
        **extra,
    )(*args)


def shape(*dims):
    return jax.ShapeDtypeStruct(dims, jnp.float32)


VMEM = pl.BlockSpec(memory_space=pltpu.VMEM)
SMEM = pl.BlockSpec(memory_space=pltpu.SMEM)


def scale_body(spot, scales, green, noise, sets, *outs):
    row_pieces, mine, theirs = outs[:8], outs[8], outs[9]
    z, y_hi, y_lo, x, core = (spot[i] for i in range(5))
    chosen = sets[...]
    factor = jnp.zeros_like(noise[...])
    for s in range(4):
        factor = jnp.where(chosen == s, scales[s], factor)
    root = jnp.broadcast_to(jnp.sqrt(noise[...] * factor), (16, 16))
    eye = lax.broadcasted_iota(jnp.int32, (16, 16), 0) == lax.broadcasted_iota(jnp.int32, (16, 16), 1)
    root = jnp.sum(jnp.where(eye, root, 0.0), axis=1, keepdims=True)
    for c in range(2):
        hi = y_hi if c == 0 else 1 - y_hi
        lo = y_lo if c == 0 else 1 - y_lo
        for d in range(4):
            start = (lax.rem(z + d, 4) * 2 + hi) * 2048
            row_pieces[c * 4 + d][...] = green[:, pl.ds(pl.multiple_of(start, 2048), 2048)] * root
            start = (lo * 4 + lax.rem(x + d, 4)) * 2048
            mine[c * 4 + d] = green[:, pl.ds(pl.multiple_of(start + core * 1024, 1024), 1024)] * root
            theirs[c * 4 + d] = green[:, pl.ds(pl.multiple_of(start + (1 - core) * 1024, 1024), 1024)] * root


def split_body(mine, other, *outs):
    for i in range(8):
        outs[i][0] = mine[i]
        outs[i][1] = other[i]


def join_rows_body(*refs):
    out = refs[8]
    for c in range(2):
        for d in range(4):
            out[(d * 2 + c) * 16 : (d * 2 + c + 1) * 16, :] = refs[c * 4 + d][...]


def join_cols_body(*refs):
    out = refs[8]
    for c in range(2):
        for d in range(4):
            for j in range(2):
                at = ((d * 2 + c) * 2 + j) * 16
                out[at : at + 16, :] = refs[c * 4 + d][j]


def exact(left, right, dims):
    return lax.dot_general(
        left, right, (dims, ((), ())), precision=lax.Precision.HIGHEST, preferred_element_type=jnp.float32
    )


def sides_body(spot, cell, stiff, row_side, col_side):
    grid = jnp.zeros((NSTRIKE, NDIP), jnp.float32)
    for i in range(8):
        part = pl.ds(i * 1024, 1024)
        cells = cell[:, part]
        strikes = lax.broadcasted_iota(jnp.int32, (NSTRIKE, 1024), 0)
        dips = lax.broadcasted_iota(jnp.int32, (NDIP, 1024), 0)
        at_strike = jnp.where(cells // NDIP == strikes, stiff[:, part], 0.0)
        at_dip = jnp.where(cells % NDIP == dips, 1.0, 0.0)
        grid = grid + exact(at_strike, at_dip, ((1,), (1,)))
    along = jnp.zeros((1, NDIP), jnp.float32)
    across = jnp.zeros((NSTRIKE, 1), jnp.float32)
    strike_ids = lax.broadcasted_iota(jnp.int32, (NSTRIKE, NDIP), 0)
    dip_ids = lax.broadcasted_iota(jnp.int32, (NSTRIKE, NDIP), 1)
    after = jnp.concatenate([grid[1:], along], 0)
    before = jnp.concatenate([along, grid[:-1]], 0)
    below = jnp.concatenate([grid[:, 1:], across], 1)
    above = jnp.concatenate([across, grid[:, :-1]], 1)
    degree = jnp.where(strike_ids < NSTRIKE - 1, 0.5 * (grid + after), 0.0)
    degree = degree + jnp.where(strike_ids > 0, 0.5 * (grid + before), 0.0)
    degree = degree + jnp.where(dip_ids < NDIP - 1, 0.5 * (grid + below), 0.0)
    degree = degree + jnp.where(dip_ids > 0, 0.5 * (grid + above), 0.0)
    first = pl.multiple_of(spot[5], 2048)
    cells = cell[:, pl.ds(first, ROWS)]
    strike = cells // NDIP
    dip = cells % NDIP
    in_strike = jnp.where(strike == lax.broadcasted_iota(jnp.int32, (NSTRIKE, ROWS), 0), 1.0, 0.0)
    by_dip = exact(degree.T, in_strike, ((1,), (0,)))
    in_dip = dip == lax.broadcasted_iota(jnp.int32, (NDIP, ROWS), 0)
    row_degree = jnp.sum(jnp.where(in_dip, by_dip, 0.0), axis=0, keepdims=True)
    row_side[0:1, :] = strike.astype(jnp.float32)
    row_side[1:2, :] = dip.astype(jnp.float32)
    row_side[2:3, :] = 0.5 * stiff[:, pl.ds(first, ROWS)]
    row_side[3:4, :] = row_degree
    row_side[4:8, :] = jnp.zeros((4, ROWS), jnp.float32)
    first = pl.multiple_of(spot[6], 1024)
    cells = cell[:, pl.ds(first, COLS)]
    col_side[0:1, :] = (cells // NDIP).astype(jnp.float32)
    col_side[1:2, :] = (cells % NDIP).astype(jnp.float32)
    col_side[2:3, :] = 0.5 * stiff[:, pl.ds(first, COLS)]
    col_side[3:8, :] = jnp.zeros((5, COLS), jnp.float32)


def prior_tile(spot, row_side, col_side):
    sides = row_side.T
    spacing = jnp.abs(sides[:, 0:1] - col_side[0:1, :]) + jnp.abs(sides[:, 1:2] - col_side[1:2, :])
    spacing = jnp.where(spot[7] == 1, spacing, 9.0)
    coupling = jnp.where(spacing == 1.0, -(sides[:, 2:3] + col_side[2:3, :]), 0.0)
    return jnp.where(spacing == 0.0, sides[:, 3:4], coupling)


def split_right(late, core, right, spots, high, low):
    depth = 32 * len(right)
    for n in range(4):
        for j in range(2):
            who = core if j == 0 else 1 - core
            dx = (0, 1 + 2 * who, 3 - 2 * who, 2)[n]
            for ref, at in zip(right, spots):
                for c in range(2):
                    c_from = 1 - c if late else c
                    source = pl.multiple_of(dx * 64 + c_from * 32 + j * 16, 16)
                    target = pl.multiple_of((j * 4 + n) * depth + at * 32 + c * 16, 16)
                    piece = ref[pl.ds(source, 16), :]
                    top = piece.astype(jnp.bfloat16)
                    high[pl.ds(target, 16), :] = top
                    low[pl.ds(target, 16), :] = (piece - top.astype(jnp.float32)).astype(jnp.bfloat16)


def product(left, rows, part, high, low):
    block = jnp.concatenate([ref[a:b, part] for ref in left for a, b in rows], 0).T
    top = block.astype(jnp.bfloat16)
    rest = (block - top.astype(jnp.float32)).astype(jnp.bfloat16)

    def dot(a, b):
        return jnp.dot(a, b, preferred_element_type=jnp.float32)

    return dot(top, high[...]) + (dot(top, low[...]) + dot(rest, high[...]))


ALL = ((0, 128),)
MOST = ((0, 64), (96, 128))
FAR = ((64, 96),)


def near_body(start, stop, spot, *refs):
    left, right = refs[:8], refs[8:12]
    row_side, col_side = refs[12:14]
    out, high, low = refs[-3:]
    core = spot[4]
    split_right(False, core, right, (0, 1 + 2 * core, 3 - 2 * core, 2), high, low)

    @pl.loop(start // TILE, stop // TILE)
    def _(i):
        part = pl.ds(pl.multiple_of(i * TILE, TILE), TILE)
        out[part, :] = product(left, ALL, part, high, low) + prior_tile(spot, row_side[:, part], col_side)


def late_body(spot, *refs):
    left, right = refs[:8], refs[8:11]
    total, out, high, low = refs[11:]
    core = spot[4]
    split_right(True, core, right, (0, 1 + core, 2 - core), high, low)

    @pl.loop(0, ROWS // TILE)
    def _(i):
        part = pl.ds(pl.multiple_of(i * TILE, TILE), TILE)
        out[part, :] = total[part, :] + product(left, MOST, part, high, low)


def far_body(spot, *refs):
    left, right = refs[:8], refs[8:9]
    total, out, high, low = refs[9:]

    @pl.when(pl.program_id(0) == 0)
    def _():
        split_right(True, spot[4], right, (0,), high, low)

    part = pl.ds(pl.multiple_of(pl.program_id(0) * TILE, TILE), TILE)
    out[...] = total[part, :] + product(left, FAR, part, high, low)


TILE = 256


def gram_call(body, depth, spot, *args, **extra):
    args = (spot, *args)
    return kernel_call(
        body,
        shape(ROWS, COLS),
        args,
        in_specs=[SMEM] + [VMEM] * (len(args) - 1),
        scratch=[pltpu.VMEM((depth, COLS), jnp.bfloat16)] * 2,
        flops=3 * 2 * ROWS * COLS * depth,
        nbytes=24 << 20,
        limit=12,
        **extra,
    )


def ring(block, axis):
    def shift(sign):
        def target(z, y, x, core):
            step = sign if core == 0 else -sign
            return (z + step, y, x, core) if axis == "z" else (z, y, x + step, core)

        return target

    first = send(block, shift(1))
    second = send(block, shift(-1))
    far = send(first, shift(1))
    return [block, first, second, far]


def swap(blocks):
    return [send(b, lambda z, y, x, core: (z, y, x, 1 - core)) for b in blocks]


def scatter(pieces, axis):
    got = []
    for c in range(2):
        for d in range(4):
            if c == 0 and d == 0:
                got.append(pieces[0])
                continue

            def target(z, y, x, core):
                to = CROSS[y] if c else y
                return (z + d, to, x, core) if axis == "z" else (z, to, x + d, core)

            got.append(send(pieces[c * 4 + d], target))
    return got


def per_device(green, noise_precision, data_set, set_scale, stiffness, patch_cell):
    row, col = lax.axis_index("row"), lax.axis_index("col")
    row_start, col_start = row * ROWS, col * COLS
    spot = jnp.stack(
        [
            row // 2,
            row % 2,
            col // 8,
            col // 2 % 4,
            col % 2,
            row_start % PATCHES,
            col_start % PATCHES,
            (row_start // PATCHES == col_start // PATCHES).astype(jnp.int32),
        ]
    ).astype(jnp.int32)
    *row_pieces, mine, theirs = kernel_call(
        scale_body,
        [shape(16, 2048)] * 8 + [shape(8, 16, 1024)] * 2,
        (spot, set_scale, green, noise_precision.reshape(1, 16), data_set.reshape(1, 16)),
        in_specs=[SMEM, SMEM, VMEM, VMEM, VMEM],
        flops=1 << 20,
        nbytes=3 << 20,
    )
    (other,) = swap([theirs])
    row_pieces = scatter(row_pieces, "z")
    col_pieces = kernel_call(split_body, [shape(2, 16, 1024)] * 8, (mine, other), flops=1 << 20, nbytes=2 << 20)
    col_pieces = scatter(col_pieces, "x")
    row_near = kernel_call(join_rows_body, shape(128, 2048), row_pieces, flops=1 << 20, nbytes=2 << 20)
    row_late = send(row_near, lambda z, y, x, core: (z, PAIR[y], x, core))
    col_near = kernel_call(join_cols_body, shape(256, 1024), col_pieces, flops=1 << 20, nbytes=2 << 20)
    col_late = send(col_near, lambda z, y, x, core: (z, DIAGONAL[y], x, core))
    sides = kernel_call(
        sides_body,
        [shape(8, ROWS), shape(8, COLS)],
        (spot, patch_cell.reshape(1, -1), stiffness.reshape(1, -1)),
        in_specs=[SMEM, VMEM, VMEM],
        flops=1 << 30,
        nbytes=1 << 20,
    )
    row_near = ring(row_near, "x")
    col_near = ring(col_near, "z")
    row_late = ring(row_late, "x")
    col_late = ring(col_late, "z")
    left = row_near + swap(row_near)
    total = gram_call(functools.partial(near_body, 0, ROWS // 2), 1024, spot, *left, *col_near, *sides)
    total = gram_call(
        functools.partial(near_body, ROWS // 2, ROWS),
        1024,
        spot,
        *left,
        *col_near,
        *sides,
        total,
        input_output_aliases={15: 0},
    )
    left = row_late + swap(row_late)
    total = gram_call(late_body, 768, spot, *left, *col_late[:3], total, input_output_aliases={12: 0})
    return gram_call(
        far_body,
        256,
        spot,
        *left,
        col_late[3],
        total,
        grid=(ROWS // TILE,),
        out_specs=pl.BlockSpec((TILE, COLS), lambda i: (i, 0)),
    )


def solution(mesh):
    placed = (P(AXES, None), P(AXES), P(AXES), P(), P(), P())

    return jax.shard_map(per_device, mesh=mesh, in_specs=placed, out_specs=P("row", "col"), check_vma=False)
```

```python
import functools

import jax
import jax.numpy as jnp
from jax import lax
from jax.experimental import pallas as pl
from jax.experimental.pallas import tpu as pltpu
from jax.sharding import PartitionSpec as P


NSTRIKE = 128
NDIP = 64
AXES = ("row", "col")
CROSS = (3, 2, 1, 0)
PAIR = (1, 0, 3, 2)
DIAGONAL = (2, 3, 0, 1)
ROWS = 2048
COLS = 1024
PATCHES = 8192


def place(index):
    row, col = divmod(index, 16)
    z, y_hi = divmod(row, 2)
    y_lo, rest = divmod(col, 8)
    x, core = divmod(rest, 2)
    return z, 2 * y_hi + y_lo, x, core


def device(z, y, x, core):
    return (z % 4 * 2 + y // 2) * 16 + (y % 2) * 8 + x % 4 * 2 + core


def send(block, target):
    pairs = [(index, device(*target(*place(index)))) for index in range(128)]
    return lax.ppermute(block, AXES, pairs)


def kernel_call(body, outs, args, in_specs=None, flops=0, nbytes=0, scratch=(), limit=6, **extra):
    return pl.pallas_call(
        body,
        out_shape=outs,
        in_specs=in_specs or [VMEM] * len(args),
        scratch_shapes=scratch,
        cost_estimate=pl.CostEstimate(flops=flops, bytes_accessed=nbytes, transcendentals=0),
        compiler_params=pltpu.CompilerParams(vmem_limit_bytes=limit << 20),
        **extra,
    )(*args)


def shape(*dims):
    return jax.ShapeDtypeStruct(dims, jnp.float32)


VMEM = pl.BlockSpec(memory_space=pltpu.VMEM)
SMEM = pl.BlockSpec(memory_space=pltpu.SMEM)
HBM = pl.BlockSpec(memory_space=pltpu.HBM)


def scale_body(spot, green, pack, *outs):
    row_pieces, mine, theirs = outs[:8], outs[8], outs[9]
    z, y_hi, y_lo, x, core = (spot[i] for i in range(5))
    noise, chosen = pack[0:1, 0:16], pack[0:1, 16:32]
    factor = jnp.zeros_like(noise)
    for s in range(4):
        factor = jnp.where(chosen == float(s), pack[0:1, 32 + s : 33 + s], factor)
    root = jnp.broadcast_to(jnp.sqrt(noise * factor), (16, 16))
    eye = lax.broadcasted_iota(jnp.int32, (16, 16), 0) == lax.broadcasted_iota(jnp.int32, (16, 16), 1)
    root = jnp.sum(jnp.where(eye, root, 0.0), axis=1, keepdims=True)
    for c in range(2):
        hi = y_hi if c == 0 else 1 - y_hi
        lo = y_lo if c == 0 else 1 - y_lo
        for d in range(4):
            start = (lax.rem(z + d, 4) * 2 + hi) * 2048
            row_pieces[c * 4 + d][...] = green[:, pl.ds(pl.multiple_of(start, 2048), 2048)] * root
            start = (lo * 4 + lax.rem(x + d, 4)) * 2048
            mine[c * 4 + d] = green[:, pl.ds(pl.multiple_of(start + core * 1024, 1024), 1024)] * root
            theirs[c * 4 + d] = green[:, pl.ds(pl.multiple_of(start + (1 - core) * 1024, 1024), 1024)] * root


def split_body(mine, other, *outs):
    for i in range(8):
        outs[i][0] = mine[i]
        outs[i][1] = other[i]


def join_rows_body(*refs):
    out = refs[8]
    for c in range(2):
        for d in range(4):
            out[(d * 2 + c) * 16 : (d * 2 + c + 1) * 16, :] = refs[c * 4 + d][...]


def join_cols_body(*refs):
    out = refs[8]
    for c in range(2):
        for d in range(4):
            for j in range(2):
                at = ((d * 2 + c) * 2 + j) * 16
                out[at : at + 16, :] = refs[c * 4 + d][j]


def exact(left, right, dims):
    return lax.dot_general(
        left, right, (dims, ((), ())), precision=lax.Precision.HIGHEST, preferred_element_type=jnp.float32
    )


def sides_body(spot, cell, stiff, row_side, col_side):
    grid = jnp.zeros((NSTRIKE, NDIP), jnp.float32)
    for i in range(8):
        part = pl.ds(i * 1024, 1024)
        cells = cell[:, part]
        strikes = lax.broadcasted_iota(jnp.int32, (NSTRIKE, 1024), 0)
        dips = lax.broadcasted_iota(jnp.int32, (NDIP, 1024), 0)
        at_strike = jnp.where(cells // NDIP == strikes, stiff[:, part], 0.0)
        at_dip = jnp.where(cells % NDIP == dips, 1.0, 0.0)
        grid = grid + exact(at_strike, at_dip, ((1,), (1,)))
    along = jnp.zeros((1, NDIP), jnp.float32)
    across = jnp.zeros((NSTRIKE, 1), jnp.float32)
    strike_ids = lax.broadcasted_iota(jnp.int32, (NSTRIKE, NDIP), 0)
    dip_ids = lax.broadcasted_iota(jnp.int32, (NSTRIKE, NDIP), 1)
    after = jnp.concatenate([grid[1:], along], 0)
    before = jnp.concatenate([along, grid[:-1]], 0)
    below = jnp.concatenate([grid[:, 1:], across], 1)
    above = jnp.concatenate([across, grid[:, :-1]], 1)
    degree = jnp.where(strike_ids < NSTRIKE - 1, 0.5 * (grid + after), 0.0)
    degree = degree + jnp.where(strike_ids > 0, 0.5 * (grid + before), 0.0)
    degree = degree + jnp.where(dip_ids < NDIP - 1, 0.5 * (grid + below), 0.0)
    degree = degree + jnp.where(dip_ids > 0, 0.5 * (grid + above), 0.0)
    first = pl.multiple_of(spot[5], 2048)
    cells = cell[:, pl.ds(first, ROWS)]
    strike = cells // NDIP
    dip = cells % NDIP
    in_strike = jnp.where(strike == lax.broadcasted_iota(jnp.int32, (NSTRIKE, ROWS), 0), 1.0, 0.0)
    by_dip = exact(degree.T, in_strike, ((1,), (0,)))
    in_dip = dip == lax.broadcasted_iota(jnp.int32, (NDIP, ROWS), 0)
    row_degree = jnp.sum(jnp.where(in_dip, by_dip, 0.0), axis=0, keepdims=True)
    row_side[0:1, :] = strike.astype(jnp.float32)
    row_side[1:2, :] = dip.astype(jnp.float32)
    row_side[2:3, :] = 0.5 * stiff[:, pl.ds(first, ROWS)]
    row_side[3:4, :] = row_degree
    row_side[4:8, :] = jnp.zeros((4, ROWS), jnp.float32)
    first = pl.multiple_of(spot[6], 1024)
    cells = cell[:, pl.ds(first, COLS)]
    col_side[0:1, :] = (cells // NDIP).astype(jnp.float32)
    col_side[1:2, :] = (cells % NDIP).astype(jnp.float32)
    col_side[2:3, :] = 0.5 * stiff[:, pl.ds(first, COLS)]
    col_side[3:8, :] = jnp.zeros((5, COLS), jnp.float32)


def prior_tile(spot, row_side, col_side):
    sides = row_side.T
    spacing = jnp.abs(sides[:, 0:1] - col_side[0:1, :]) + jnp.abs(sides[:, 1:2] - col_side[1:2, :])
    spacing = jnp.where(spot[7] == 1, spacing, 9.0)
    coupling = jnp.where(spacing == 1.0, -(sides[:, 2:3] + col_side[2:3, :]), 0.0)
    return jnp.where(spacing == 0.0, sides[:, 3:4], coupling)


EARLY = ((0, 1, 3), (0, 1, 3), (0, 1, 3), (), (0, 1, 3), (1, 3), (1, 3), ())
REST = ((2,), (2,), (2,), (0, 1, 2, 3), (2,), (0, 2), (0, 2), (0, 1, 2, 3))
TILE = 256


def split_right(late, plan, core, right, high, low):
    start = 0
    for i, chosen in enumerate(plan):
        who = core if i < 4 else 1 - core
        dx = (0, 1 + 2 * who, 3 - 2 * who, 2)[i % 4]
        at = {dz: start + 32 * k for k, dz in enumerate(chosen)}
        targets = []
        if 0 in at:
            targets.append((0, at[0]))
        if 1 in at:
            targets.append((1, at[1] + core * (at[3] - at[1])))
            targets.append((2, at[3] + core * (at[1] - at[3])))
        if 2 in at:
            targets.append((3, at[2]))
        for m, base in targets:
            for c in range(2):
                c_from = 1 - c if late else c
                source = pl.multiple_of(dx * 64 + c_from * 32 + i // 4 * 16, 16)
                target = pl.multiple_of(base + c * 16, 16)
                piece = right[m][pl.ds(source, 16), :]
                top = piece.astype(jnp.bfloat16)
                high[pl.ds(target, 16), :] = top
                low[pl.ds(target, 16), :] = (piece - top.astype(jnp.float32)).astype(jnp.bfloat16)
        start += 32 * len(chosen)


def product(left, plan, part, high, low):
    refs = iter(left)
    rows = []
    for chosen in plan:
        if chosen:
            ref = next(refs)
            rows += [ref[dz * 32 : dz * 32 + 32, part] for dz in chosen]
    block = jnp.concatenate(rows, 0).T
    top = block.astype(jnp.bfloat16)
    rest = (block - top.astype(jnp.float32)).astype(jnp.bfloat16)

    def dot(a, b):
        return jnp.dot(a, b, preferred_element_type=jnp.float32)

    return dot(top, high[...]) + (dot(top, low[...]) + dot(rest, high[...]))


def gram_body(plan, late, last, spot, *refs):
    n_left = sum(1 for chosen in plan if chosen)
    n_right = 3 if plan is EARLY else 4
    left, right = refs[:n_left], refs[n_left : n_left + n_right]
    if last:
        *extra, result, high, low, out, sent = refs[n_left + n_right :]
    else:
        *extra, out, high, low = refs[n_left + n_right :]
    split_right(late, plan, spot[4], right, high, low)

    def copy(i):
        part = pl.ds(pl.multiple_of(i * TILE, TILE), TILE)
        return pltpu.make_async_copy(out.at[part, :], result.at[part, :], sent.at[i])

    @pl.loop(0, ROWS // TILE, unroll=UNROLL)
    def _(i):
        part = pl.ds(pl.multiple_of(i * TILE, TILE), TILE)
        block = product(left, plan, part, high, low)
        if len(extra) == 1:
            out[part, :] = extra[0][part, :] + block
        else:
            out[part, :] = block + prior_tile(spot, extra[0][:, part], extra[1])
        if last:
            copy(i).start()

    if last:
        for i in range(ROWS // TILE):
            copy(i).wait()


UNROLL = 4


def gram_call(plan, late, last, spot, left, right, extra):
    left = [ref for ref, chosen in zip(left, plan) if chosen]
    right = right[:3] if plan is EARLY else right
    depth = 32 * sum(len(chosen) for chosen in plan)
    args = (spot, *left, *right, *extra)
    options = {}
    scratch = [pltpu.VMEM((depth, COLS), jnp.bfloat16)] * 2
    if last:
        options = dict(out_specs=HBM)
        scratch += [pltpu.VMEM((ROWS, COLS), jnp.float32), pltpu.SemaphoreType.DMA((ROWS // TILE,))]
    elif len(extra) == 1:
        options = dict(input_output_aliases={len(args) - 1: 0})
    return kernel_call(
        functools.partial(gram_body, plan, late, last),
        shape(ROWS, COLS),
        args,
        in_specs=[SMEM] + [VMEM] * (len(args) - 1),
        scratch=scratch,
        flops=3 * 2 * ROWS * COLS * depth,
        nbytes=24 << 20,
        limit=20 if last else 12,
        **options,
    )


def ring(block, axis, across=None):
    def shift(sign):
        def target(z, y, x, core):
            step = sign if core == 0 else -sign
            return (z + step, y, x, core) if axis == "z" else (z, y, x + step, core)

        return target

    first = send(block, shift(1))
    second = send(block, shift(-1))
    if across is None:
        far = send(first, shift(1))
    else:
        far = send(across, lambda z, y, x, core: (z, DIAGONAL[y], x, core))
    return [block, first, second, far]


def swap(blocks):
    return [send(b, lambda z, y, x, core: (z, y, x, 1 - core)) for b in blocks]


def scatter(pieces, axis):
    got = []
    for c in range(2):
        for d in range(4):
            if c == 0 and d == 0:
                got.append(pieces[0])
                continue

            def target(z, y, x, core):
                to = CROSS[y] if c else y
                return (z + d, to, x, core) if axis == "z" else (z, to, x + d, core)

            got.append(send(pieces[c * 4 + d], target))
    return got


def per_device(green, noise_precision, data_set, set_scale, stiffness, patch_cell):
    row, col = lax.axis_index("row"), lax.axis_index("col")
    row_start, col_start = row * ROWS, col * COLS
    spot = jnp.stack(
        [
            row // 2,
            row % 2,
            col // 8,
            col // 2 % 4,
            col % 2,
            row_start % PATCHES,
            col_start % PATCHES,
            (row_start // PATCHES == col_start // PATCHES).astype(jnp.int32),
        ]
    ).astype(jnp.int32)
    pack = jnp.concatenate([noise_precision, data_set.astype(jnp.float32), set_scale, jnp.zeros((92,), jnp.float32)])
    *row_pieces, mine, theirs = kernel_call(
        scale_body,
        [shape(16, 2048)] * 8 + [shape(8, 16, 1024)] * 2,
        (spot, green, pack.reshape(1, -1)),
        in_specs=[SMEM, VMEM, VMEM],
        flops=1 << 20,
        nbytes=3 << 20,
    )
    (other,) = swap([theirs])
    row_pieces = scatter(row_pieces, "z")
    col_pieces = kernel_call(split_body, [shape(2, 16, 1024)] * 8, (mine, other), flops=1 << 20, nbytes=2 << 20)
    col_pieces = scatter(col_pieces, "x")
    row_near = kernel_call(join_rows_body, shape(128, 2048), row_pieces, flops=1 << 20, nbytes=2 << 20)
    row_late = send(row_near, lambda z, y, x, core: (z, PAIR[y], x, core))
    col_near = kernel_call(join_cols_body, shape(256, 1024), col_pieces, flops=1 << 20, nbytes=2 << 20)
    col_late = send(col_near, lambda z, y, x, core: (z, DIAGONAL[y], x, core))
    sides = kernel_call(
        sides_body,
        [shape(8, ROWS), shape(8, COLS)],
        (spot, patch_cell.reshape(1, -1), stiffness.reshape(1, -1)),
        in_specs=[SMEM, VMEM, VMEM],
        flops=1 << 30,
        nbytes=1 << 20,
    )
    row_near = ring(row_near, "x")
    col_near = ring(col_near, "z")
    row_late = ring(row_late, "x")
    col_late = ring(col_late, "z", col_near[3])
    left = row_near + swap(row_near)
    total = gram_call(EARLY, False, False, spot, left, col_near, sides)
    total = gram_call(REST, False, False, spot, left, col_near, [total])
    left = row_late + swap(row_late)
    total = gram_call(EARLY, True, False, spot, left, col_late, [total])
    return gram_call(REST, True, True, spot, left, col_late, [total])


def solution(mesh):
    placed = (P(AXES, None), P(AXES), P(AXES), P(), P(), P())

    return jax.shard_map(per_device, mesh=mesh, in_specs=placed, out_specs=P("row", "col"), check_vma=False)
```

```python
import functools

import jax
import jax.numpy as jnp
from jax import lax
from jax.experimental import pallas as pl
from jax.experimental.pallas import tpu as pltpu
from jax.sharding import PartitionSpec as P


NSTRIKE = 128
NDIP = 64
AXES = ("row", "col")
CROSS = (3, 2, 1, 0)
PAIR = (1, 0, 3, 2)
DIAGONAL = (2, 3, 0, 1)
ROWS = 2048
COLS = 1024
PATCHES = 8192


def place(index):
    row, col = divmod(index, 16)
    z, y_hi = divmod(row, 2)
    y_lo, rest = divmod(col, 8)
    x, core = divmod(rest, 2)
    return z, 2 * y_hi + y_lo, x, core


def device(z, y, x, core):
    return (z % 4 * 2 + y // 2) * 16 + (y % 2) * 8 + x % 4 * 2 + core


def send(block, target):
    pairs = [(index, device(*target(*place(index)))) for index in range(128)]
    return lax.ppermute(block, AXES, pairs)


def kernel_call(body, outs, args, in_specs=None, flops=0, nbytes=0, scratch=(), limit=6, **extra):
    return pl.pallas_call(
        body,
        out_shape=outs,
        in_specs=in_specs or [VMEM] * len(args),
        scratch_shapes=scratch,
        cost_estimate=pl.CostEstimate(flops=flops, bytes_accessed=nbytes, transcendentals=0),
        compiler_params=pltpu.CompilerParams(vmem_limit_bytes=limit << 20),
        **extra,
    )(*args)


def shape(*dims):
    return jax.ShapeDtypeStruct(dims, jnp.float32)


VMEM = pl.BlockSpec(memory_space=pltpu.VMEM)
SMEM = pl.BlockSpec(memory_space=pltpu.SMEM)
HBM = pl.BlockSpec(memory_space=pltpu.HBM)


def scale_body(spot, green, weight, *outs):
    row_pieces, mine, theirs = outs[:8], outs[8], outs[9]
    z, y_hi, y_lo, x, core = (spot[i] for i in range(5))
    root = jnp.broadcast_to(jnp.sqrt(weight[...]), (16, 16))
    eye = lax.broadcasted_iota(jnp.int32, (16, 16), 0) == lax.broadcasted_iota(jnp.int32, (16, 16), 1)
    root = jnp.sum(jnp.where(eye, root, 0.0), axis=1, keepdims=True)
    for c in range(2):
        hi = y_hi if c == 0 else 1 - y_hi
        lo = y_lo if c == 0 else 1 - y_lo
        for d in range(4):
            start = (lax.rem(z + d, 4) * 2 + hi) * 2048
            row_pieces[c * 4 + d][...] = green[:, pl.ds(pl.multiple_of(start, 2048), 2048)] * root
            start = (lo * 4 + lax.rem(x + d, 4)) * 2048
            mine[c * 4 + d] = green[:, pl.ds(pl.multiple_of(start + core * 1024, 1024), 1024)] * root
            theirs[c * 4 + d] = green[:, pl.ds(pl.multiple_of(start + (1 - core) * 1024, 1024), 1024)] * root


def split_body(mine, other, *outs):
    for i in range(8):
        outs[i][0] = mine[i]
        outs[i][1] = other[i]


def join_rows_body(*refs):
    out = refs[8]
    for c in range(2):
        for d in range(4):
            out[(d * 2 + c) * 16 : (d * 2 + c + 1) * 16, :] = refs[c * 4 + d][...]


def join_cols_body(*refs):
    out = refs[8]
    for c in range(2):
        for d in range(4):
            for j in range(2):
                at = ((d * 2 + c) * 2 + j) * 16
                out[at : at + 16, :] = refs[c * 4 + d][j]


def exact(left, right, dims):
    return lax.dot_general(
        left, right, (dims, ((), ())), precision=lax.Precision.HIGHEST, preferred_element_type=jnp.float32
    )


def sides_body(spot, cell, stiff, row_side, col_side):
    grid = jnp.zeros((NSTRIKE, NDIP), jnp.float32)
    for i in range(8):
        part = pl.ds(i * 1024, 1024)
        cells = cell[:, part]
        strikes = lax.broadcasted_iota(jnp.int32, (NSTRIKE, 1024), 0)
        dips = lax.broadcasted_iota(jnp.int32, (NDIP, 1024), 0)
        at_strike = jnp.where(cells // NDIP == strikes, stiff[:, part], 0.0)
        at_dip = jnp.where(cells % NDIP == dips, 1.0, 0.0)
        grid = grid + exact(at_strike, at_dip, ((1,), (1,)))
    along = jnp.zeros((1, NDIP), jnp.float32)
    across = jnp.zeros((NSTRIKE, 1), jnp.float32)
    strike_ids = lax.broadcasted_iota(jnp.int32, (NSTRIKE, NDIP), 0)
    dip_ids = lax.broadcasted_iota(jnp.int32, (NSTRIKE, NDIP), 1)
    after = jnp.concatenate([grid[1:], along], 0)
    before = jnp.concatenate([along, grid[:-1]], 0)
    below = jnp.concatenate([grid[:, 1:], across], 1)
    above = jnp.concatenate([across, grid[:, :-1]], 1)
    degree = jnp.where(strike_ids < NSTRIKE - 1, 0.5 * (grid + after), 0.0)
    degree = degree + jnp.where(strike_ids > 0, 0.5 * (grid + before), 0.0)
    degree = degree + jnp.where(dip_ids < NDIP - 1, 0.5 * (grid + below), 0.0)
    degree = degree + jnp.where(dip_ids > 0, 0.5 * (grid + above), 0.0)
    first = pl.multiple_of(spot[5], 2048)
    cells = cell[:, pl.ds(first, ROWS)]
    strike = cells // NDIP
    dip = cells % NDIP
    in_strike = jnp.where(strike == lax.broadcasted_iota(jnp.int32, (NSTRIKE, ROWS), 0), 1.0, 0.0)
    by_dip = exact(degree.T, in_strike, ((1,), (0,)))
    in_dip = dip == lax.broadcasted_iota(jnp.int32, (NDIP, ROWS), 0)
    row_degree = jnp.sum(jnp.where(in_dip, by_dip, 0.0), axis=0, keepdims=True)
    row_side[0:1, :] = strike.astype(jnp.float32)
    row_side[1:2, :] = dip.astype(jnp.float32)
    row_side[2:3, :] = 0.5 * stiff[:, pl.ds(first, ROWS)]
    row_side[3:4, :] = row_degree
    row_side[4:8, :] = jnp.zeros((4, ROWS), jnp.float32)
    first = pl.multiple_of(spot[6], 1024)
    cells = cell[:, pl.ds(first, COLS)]
    col_side[0:1, :] = (cells // NDIP).astype(jnp.float32)
    col_side[1:2, :] = (cells % NDIP).astype(jnp.float32)
    col_side[2:3, :] = 0.5 * stiff[:, pl.ds(first, COLS)]
    col_side[3:8, :] = jnp.zeros((5, COLS), jnp.float32)


def prior_tile(spot, row_side, col_side):
    sides = row_side.T
    spacing = jnp.abs(sides[:, 0:1] - col_side[0:1, :]) + jnp.abs(sides[:, 1:2] - col_side[1:2, :])
    spacing = jnp.where(spot[7] == 1, spacing, 9.0)
    coupling = jnp.where(spacing == 1.0, -(sides[:, 2:3] + col_side[2:3, :]), 0.0)
    return jnp.where(spacing == 0.0, sides[:, 3:4], coupling)


EARLY = ((0, 1, 2), (0, 1, 2), (0, 1, 2), (), (0, 1, 2), (1, 2), (1, 2), ())
REST = ((3,), (3,), (3,), (0, 1, 2, 3), (3,), (0, 3), (0, 3), (0, 1, 2, 3))
LATE = ((0, 1), (0, 1), (0, 1), (), (0, 1), (), (), ())
LATER = ((2, 3), (2, 3), (2, 3), (), (2, 3), (0, 1, 2, 3), (0, 1, 2, 3), ())
LAST = ((), (), (), (0, 1, 2, 3), (), (), (), (0, 1, 2, 3))
TILE = 256


def offsets(core):
    return (0, 1 + 2 * core, 3 - 2 * core, 2)


def blocks_of(plan):
    return sorted(set(sum(plan, ())))


def split_right(late, plan, core, right, high, low):
    refs = dict(zip(blocks_of(plan), right))
    target = 0
    for i, chosen in enumerate(plan):
        dx = offsets(core if i < 4 else 1 - core)[i % 4]
        for m in chosen:
            for c in range(2):
                c_from = 1 - c if late else c
                source = pl.multiple_of(dx * 64 + c_from * 32 + i // 4 * 16, 16)
                piece = refs[m][pl.ds(source, 16), :]
                top = piece.astype(jnp.bfloat16)
                high[target : target + 16, :] = top
                low[target : target + 16, :] = (piece - top.astype(jnp.float32)).astype(jnp.bfloat16)
                target += 16


def product(core, left, plan, part, high, low):
    refs = iter(left)
    rows = []
    for chosen in plan:
        if chosen:
            ref = next(refs)
            rows += [ref[pl.ds(pl.multiple_of(offsets(core)[m] * 32, 32), 32), part] for m in chosen]
    block = jnp.concatenate(rows, 0).T
    top = block.astype(jnp.bfloat16)
    rest = (block - top.astype(jnp.float32)).astype(jnp.bfloat16)

    def dot(a, b):
        return jnp.dot(a, b, preferred_element_type=jnp.float32)

    return dot(top, high[...]) + (dot(top, low[...]) + dot(rest, high[...]))


def gram_body(plan, late, last, spot, *refs):
    n_left = sum(1 for chosen in plan if chosen)
    n_right = len(blocks_of(plan))
    left, right = refs[:n_left], refs[n_left : n_left + n_right]
    if last:
        *extra, result, high, low, out, sent = refs[n_left + n_right :]
    else:
        *extra, out, high, low = refs[n_left + n_right :]
    split_right(late, plan, spot[4], right, high, low)

    def copy(i):
        part = pl.ds(pl.multiple_of(i * TILE, TILE), TILE)
        return pltpu.make_async_copy(out.at[part, :], result.at[part, :], sent.at[i])

    @pl.loop(0, ROWS // TILE, unroll=8 if plan in (LATER, LAST) else UNROLL)
    def _(i):
        part = pl.ds(pl.multiple_of(i * TILE, TILE), TILE)
        block = product(spot[4], left, plan, part, high, low)
        if len(extra) == 1:
            out[part, :] = extra[0][part, :] + block
        else:
            out[part, :] = block + prior_tile(spot, extra[0][:, part], extra[1])
        if last:
            copy(i).start()

    if last:
        for i in range(ROWS // TILE):
            copy(i).wait()


UNROLL = 4


def gram_call(plan, late, last, spot, left, right, extra):
    left = [ref for ref, chosen in zip(left, plan) if chosen]
    right = [right[m] for m in blocks_of(plan)]
    depth = 32 * sum(len(chosen) for chosen in plan)
    args = (spot, *left, *right, *extra)
    options = {}
    scratch = [pltpu.VMEM((depth, COLS), jnp.bfloat16)] * 2
    if last:
        options = dict(out_specs=HBM)
        scratch += [pltpu.VMEM((ROWS, COLS), jnp.float32), pltpu.SemaphoreType.DMA((ROWS // TILE,))]
    elif len(extra) == 1:
        options = dict(input_output_aliases={len(args) - 1: 0})
    return kernel_call(
        functools.partial(gram_body, plan, late, last),
        shape(ROWS, COLS),
        args,
        in_specs=[SMEM] + [VMEM] * (len(args) - 1),
        scratch=scratch,
        flops=3 * 2 * ROWS * COLS * depth,
        nbytes=24 << 20,
        limit=20 if last else 12,
        **options,
    )


def ring(block, axis, across=None):
    def shift(sign):
        def target(z, y, x, core):
            step = sign if core == 0 else -sign
            return (z + step, y, x, core) if axis == "z" else (z, y, x + step, core)

        return target

    first = send(block, shift(1))
    second = send(block, shift(-1))
    if across is None:
        far = send(first, shift(1))
    else:
        far = send(across, lambda z, y, x, core: (z, DIAGONAL[y], x, core))
    return [block, first, second, far]


def swap(blocks):
    return [send(b, lambda z, y, x, core: (z, y, x, 1 - core)) for b in blocks]


def scatter(pieces, axis):
    got = []
    for c in range(2):
        for d in range(4):
            if c == 0 and d == 0:
                got.append(pieces[0])
                continue

            def target(z, y, x, core):
                to = CROSS[y] if c else y
                return (z + d, to, x, core) if axis == "z" else (z, to, x + d, core)

            got.append(send(pieces[c * 4 + d], target))
    return got


def per_device(green, noise_precision, data_set, set_scale, stiffness, patch_cell):
    row, col = lax.axis_index("row"), lax.axis_index("col")
    row_start, col_start = row * ROWS, col * COLS
    spot = jnp.stack(
        [
            row // 2,
            row % 2,
            col // 8,
            col // 2 % 4,
            col % 2,
            row_start % PATCHES,
            col_start % PATCHES,
            (row_start // PATCHES == col_start // PATCHES).astype(jnp.int32),
        ]
    ).astype(jnp.int32)
    matches = data_set[:, None] == jnp.arange(set_scale.shape[0], dtype=jnp.int32)[None, :]
    weight = jnp.sum(jnp.where(matches, noise_precision[:, None] * set_scale[None, :], 0.0), axis=1)
    *row_pieces, mine, theirs = kernel_call(
        scale_body,
        [shape(16, 2048)] * 8 + [shape(8, 16, 1024)] * 2,
        (spot, green, weight.reshape(1, 16)),
        in_specs=[SMEM, VMEM, VMEM],
        flops=1 << 20,
        nbytes=3 << 20,
    )
    (other,) = swap([theirs])
    row_pieces = scatter(row_pieces, "z")
    col_pieces = kernel_call(split_body, [shape(2, 16, 1024)] * 8, (mine, other), flops=1 << 20, nbytes=2 << 20)
    col_pieces = scatter(col_pieces, "x")
    row_near = kernel_call(join_rows_body, shape(128, 2048), row_pieces, flops=1 << 20, nbytes=2 << 20)
    row_late = send(row_near, lambda z, y, x, core: (z, PAIR[y], x, core))
    col_near = kernel_call(join_cols_body, shape(256, 1024), col_pieces, flops=1 << 20, nbytes=2 << 20)
    col_late = send(col_near, lambda z, y, x, core: (z, DIAGONAL[y], x, core))
    sides = kernel_call(
        sides_body,
        [shape(8, ROWS), shape(8, COLS)],
        (spot, patch_cell.reshape(1, -1), stiffness.reshape(1, -1)),
        in_specs=[SMEM, VMEM, VMEM],
        flops=1 << 30,
        nbytes=1 << 20,
    )
    row_near = ring(row_near, "x")
    col_near = ring(col_near, "z")
    row_late = ring(row_late, "x")
    col_late = ring(col_late, "z", col_near[3])
    left = row_near + swap(row_near)
    total = gram_call(EARLY, False, False, spot, left, col_near, sides)
    total = gram_call(REST, False, False, spot, left, col_near, [total])
    left = row_late + swap(row_late)
    total = gram_call(LATE, True, False, spot, left, col_late, [total])
    total = gram_call(LATER, True, False, spot, left, col_late, [total])
    return gram_call(LAST, True, True, spot, left, col_late, [total])


def solution(mesh):
    placed = (P(AXES, None), P(AXES), P(AXES), P(), P(), P())

    return jax.shard_map(per_device, mesh=mesh, in_specs=placed, out_specs=P("row", "col"), check_vma=False)
```
